32 devices in a mesh: replica: 4 (over y, core), fsdp: 8 (over z, x).
Axes of the slice: x: 2, y: 2, z: 4, core: 2. Of those that a mesh axis runs over, the one named last changes fastest.
Arguments:
- momentum: float32 [4, 64, 14336], P('replica', 'fsdp'), may hold values from -6 to 6
- gradient: bfloat16 [4, 64, 14336], P('replica', 'fsdp'), may hold values from -6 to 6
- selection: int32 [4, 1, 224, 2], replicated, may hold values from 0 to 63, as said below
Outputs:
- residual_momentum: float32 [4, 64, 14336], P('replica', 'fsdp')
- update: float32 [64, 14336], P(None, 'fsdp')
The draws below stay inside these ranges and needn't reach their ends.
Inputs may be any that keep to these rules, and one draw needn't show every extreme that they name: `selection`: for each replica and span, the 2 block numbers are distinct.
All inputs are finite; a program needn't handle non-finite values.
Results may differ from the reference program's by a relative error of at most 0.0003.
Values sent between devices are 32-bit elements; how exact they have to be, the bound alone decides.
No kernel may reach another device: no remote copies, remote signals or barrier semaphores. Data moves between devices by JAX's collectives and lax.ppermute only.
A program may use at most 64 MiB of HBM per device.

```python
import jax
import jax.numpy as jnp
from jax import lax

COLUMNS = 14336
SPAN_SIDE = 64
BLOCK_SIDE = 8
BLOCKS_KEPT = 2
REPLICAS = 4
ROWS_ALL = 64
SPAN_ROWS = 1
SPAN_COLS = 224
BLOCKS = 64


def draw_selection(key, part):
    scores = jax.random.randint(key, (REPLICAS, SPAN_ROWS, SPAN_COLS, BLOCKS), 0, 1048576)
    scores = scores * BLOCKS + jnp.arange(BLOCKS, dtype=jnp.int32)
    order = jnp.argsort(scores, axis=-1)
    return order[..., :BLOCKS_KEPT].astype(jnp.int32)


def levels(rng, shape, cuts, least, largest):
    def one(axis_at, parts):
        draws = jax.random.uniform(jax.random.fold_in(jax.random.fold_in(rng, 6), axis_at), (parts,), jnp.float32, least / len(cuts), largest / len(cuts))
        return jnp.repeat(jnp.exp(draws), shape[axis_at] // parts).reshape((-1,) + (1,) * (len(shape) - axis_at - 1))

    level = one(*cuts[0])
    for cut in cuts[1:]:
        level = level * one(*cut)
    return level


def gaussian(stream_key, extent, scale, limit, pieces=(), held_as=jnp.bfloat16):
    level = levels(stream_key, extent, pieces, -0.22, 0.18) if pieces else 1.0
    array = jax.random.normal(stream_key, extent, jnp.float32) * scale * level
    return jnp.minimum(jnp.maximum(array, -limit), limit).astype(held_as)


def setup_inputs(seed: int = 0) -> dict:
    keys = jax.random.split(jax.random.key(seed), 4)
    return {
        "momentum": gaussian(keys[0], (REPLICAS, ROWS_ALL, COLUMNS), 1.0, 6.0, ((0, 4), (1, 8)), jnp.float32),
        "gradient": gaussian(keys[1], (REPLICAS, ROWS_ALL, COLUMNS), 1.0, 6.0, ((0, 4), (1, 8))),
        "selection": draw_selection(jax.random.fold_in(keys[3], 71), 0),
    }


decay_rate = 0.9
highest = lax.Precision.HIGHEST

def cosine_table(side):
    freq = jnp.arange(side, dtype=jnp.float32)[:, None]
    place = jnp.arange(side, dtype=jnp.float32)[None, :]
    scale = jnp.where(freq == 0, jnp.sqrt(1.0 / side), jnp.sqrt(2.0 / side))
    return scale * jnp.cos(jnp.pi * (2.0 * place + 1.0) * freq / (2.0 * side))

def block_mask(chosen):
    per_side = SPAN_SIDE // BLOCK_SIDE
    marks = (chosen[..., None] == jnp.arange(per_side * per_side, dtype=jnp.int32)).astype(jnp.float32)
    flags = lax.optimization_barrier(jnp.sum(marks, axis=-2))
    rows_c, cols_c = flags.shape[:2]
    grid = flags.reshape(rows_c, cols_c, per_side, 1, per_side, 1)
    grid = jnp.broadcast_to(grid, (rows_c, cols_c, per_side, BLOCK_SIDE, per_side, BLOCK_SIDE))
    return grid.reshape(rows_c, cols_c, SPAN_SIDE, SPAN_SIDE)

def reference(momentum, gradient, selection):
    table = cosine_table(SPAN_SIDE)

    def one_replica(total, items):
        moment, grad, chosen = items
        decayed = decay_rate * moment + grad.astype(jnp.float32)
        spans = decayed.reshape(SPAN_ROWS, SPAN_SIDE, SPAN_COLS, SPAN_SIDE)
        coeffs = jnp.einsum('ia,racb,jb->rcij', table, spans, table, precision=highest)
        kept = coeffs * block_mask(chosen)
        spatial = jnp.einsum('ia,rcij,jb->racb', table, kept, table, precision=highest)
        return (total + kept, decayed - spatial.reshape(ROWS_ALL, COLUMNS))
    start = jnp.zeros((SPAN_ROWS, SPAN_COLS, SPAN_SIDE, SPAN_SIDE), jnp.float32)
    total, residual_momentum = lax.scan(one_replica, start, (momentum, gradient, selection))
    update = jnp.einsum('ia,rcij,jb->racb', table, total, table, precision=highest)
    return (residual_momentum, update.reshape(ROWS_ALL, COLUMNS))
```

```python
import functools
import math

import jax
import jax.numpy as jnp
import numpy as np
from jax import lax
from jax.experimental import pallas as pl
from jax.experimental.pallas import tpu as pltpu
from jax.sharding import PartitionSpec as P

SPAN_SIDE = 64
BLOCK_SIDE = 8
BLOCKS_KEPT = 2
PER_SIDE = SPAN_SIDE // BLOCK_SIDE
SLOT = BLOCKS_KEPT * BLOCK_SIDE
LANES = 128
WIDE = 256
SPANS_VREG = LANES // SLOT
TILE_SPANS = LANES // SPAN_SIDE
PARTS = 4

decay_rate = 0.9


def cosine_table():
    freq = np.arange(SPAN_SIDE, dtype=np.float64)[:, None]
    place = np.arange(SPAN_SIDE, dtype=np.float64)[None, :]
    scale = np.where(freq == 0, np.sqrt(1.0 / SPAN_SIDE), np.sqrt(2.0 / SPAN_SIDE))
    return scale * np.cos(np.pi * (2.0 * place + 1.0) * freq / (2.0 * SPAN_SIDE))


def np_split(x):
    high = x.astype(np.float32).astype(jnp.bfloat16)
    low = (x - high.astype(np.float64)).astype(np.float32).astype(jnp.bfloat16)
    return np.stack([high, low])


def tables(rows_dev):
    cosine = cosine_table()
    blocks = np.kron(np.eye(WIDE // SPAN_SIDE), cosine)
    group = SPAN_SIDE // rows_dev
    cut = cosine.reshape(PER_SIDE, BLOCK_SIDE, group, rows_dev)
    ahead = np.zeros((group, BLOCK_SIDE, LANES), np.float32)
    ahead[:, :, : rows_dev * PER_SIDE] = cut.transpose(2, 1, 3, 0).reshape(group, BLOCK_SIDE, -1)
    back = np.zeros((group, rows_dev, LANES), np.float32)
    back[:, :, :SPAN_SIDE] = cut.transpose(2, 3, 1, 0).reshape(group, rows_dev, -1)
    return np_split(blocks.T), np_split(blocks), np_split(cosine.T), ahead, back


def split(x):
    high = x.astype(jnp.bfloat16)
    low = (x - high.astype(jnp.float32)).astype(jnp.bfloat16)
    return high, low


def dot3(left, right):
    dot = functools.partial(jnp.dot, preferred_element_type=jnp.float32)
    return dot(left[0], right[0]) + (dot(left[1], right[0]) + dot(left[0], right[1]))


def take(x, index):
    return jnp.take_along_axis(x, index, axis=1, mode="promise_in_bounds")


def lane():
    return lax.broadcasted_iota(jnp.int32, (BLOCK_SIDE, LANES), 1)


def selection_rows(sel):
    count = sel.shape[1]
    full = -(-count // LANES) * LANES
    rows = []
    for k in range(BLOCKS_KEPT):
        row = sel[k : k + 1, :]
        if full != count:
            row = jnp.concatenate([row, jnp.zeros((1, full - count), jnp.int32)], axis=1)
        row = jnp.broadcast_to(row, (BLOCK_SIDE, full))
        rows.append([row[:, i : i + LANES] for i in range(0, full, LANES)])
    return rows


def spread(row, first, offset, last):
    at = first + offset
    low, high = first // LANES, last // LANES
    value = take(row[low], at & (LANES - 1))
    if high != low:
        value = jnp.where(at >= high * LANES, take(row[high], at & (LANES - 1)), value)
    return value


def slots(rows, first, count):
    at = lane()
    offset = jnp.minimum(at // SLOT, count - 1)
    parts = [spread(rows[k], first, offset, first + count - 1) for k in range(BLOCKS_KEPT)]
    return jnp.where((at // BLOCK_SIDE) % BLOCKS_KEPT == 0, parts[0], parts[1])


def vregs_of(span_cols):
    return [(s, min(SPANS_VREG, span_cols - s)) for s in range(0, span_cols, SPANS_VREG)]


def forward_kernel(
    fsdp_count, momentum, gradient, sel_ref, wide_ref, table_ref, out, decayed, moment, grad, coeffs, sems
):
    rows_dev, width = decayed.shape
    rank = lax.axis_index("fsdp")
    replica = lax.axis_index("replica")
    group = SPAN_SIDE // rows_dev
    span_row, row_block = rank // group, rank % group
    part = width // PARTS
    copies = []
    for p in range(PARTS):
        cut = (slice(None), pl.ds(p * part, part))
        for n, (src, dst) in enumerate(((momentum, moment), (gradient, grad))):
            copies.append(pltpu.make_async_copy(src.at[cut], dst.at[cut], sems.at[n, p]))
            copies[-1].start()
    table = table_ref[row_block]
    wide = (wide_ref[0], wide_ref[1])
    rows = selection_rows(sel_ref[replica, span_row])
    stack = part // WIDE * rows_dev
    all_cols = width // SPAN_SIDE
    span_cols = all_cols // fsdp_count
    at = lane()
    parity = rank % 2
    for p in range(PARTS):
        copies[2 * p].wait()
        copies[2 * p + 1].wait()
        cut = (slice(None), slice(p * part, (p + 1) * part))
        now = decay_rate * moment[cut] + grad[cut].astype(jnp.float32)
        decayed[cut] = now
        tall = jnp.concatenate([now[:, i : i + WIDE] for i in range(0, part, WIDE)], axis=0)
        coeffs[p * stack : (p + 1) * stack, :] = dot3(split(tall), wide)
    for c in range(fsdp_count):
        for j, (start, count) in enumerate(vregs_of(span_cols)):
            first = c * span_cols + start
            number = slots(rows, first, count)
            index = (number % PER_SIDE) * BLOCK_SIDE + at % BLOCK_SIDE
            index = index + ((first + at // SLOT) % TILE_SPANS) * SPAN_SIDE
            picked = None
            for tile in range(first // TILE_SPANS, (first + count - 1) // TILE_SPANS + 1):
                block, half = divmod(tile, WIDE // LANES)
                value = coeffs[block * rows_dev : (block + 1) * rows_dev, half * LANES : (half + 1) * LANES]
                value = take(value, index)
                picked = value if picked is None else jnp.where(
                    first + at // SLOT >= tile * TILE_SPANS, value, picked
                )
            where = number // PER_SIDE
            total = None
            for a in range(rows_dev):
                term = take(table, a * PER_SIDE + where) * jnp.broadcast_to(picked[a : a + 1, :], at.shape)
                total = term if total is None else total + term
            out[(c % 2) ^ parity, c // 2, :, j * LANES : (j + 1) * LANES] = total


def residual_kernel(fsdp_count, decayed, own, other, sel_ref, wide_ref, table_ref, out, coeffs, result, sems):
    rows_dev, width = decayed.shape
    rank = lax.axis_index("fsdp")
    replica = lax.axis_index("replica")
    group = SPAN_SIDE // rows_dev
    span_row, row_block = rank // group, rank % group
    part = width // PARTS
    table = table_ref[row_block]
    wide = (wide_ref[0], wide_ref[1])
    rows = selection_rows(sel_ref[replica, span_row])
    stack = part // WIDE * rows_dev
    span_cols = width // SPAN_SIDE // fsdp_count
    at = lane()
    parity = rank % 2
    packed = {}

    def vreg(c, j):
        if (c, j) not in packed:
            start, count = vregs_of(span_cols)[j]
            first = c * span_cols + start
            where = slots(rows, first, count) // PER_SIDE
            cut = (c // 2, slice(None), slice(j * LANES, (j + 1) * LANES))
            kept = jnp.where(parity == c % 2, own[cut], other[cut])
            total = None
            for i in range(BLOCK_SIDE):
                term = take(table, i * PER_SIDE + where) * jnp.broadcast_to(kept[i : i + 1, :], at.shape)
                total = term if total is None else total + term
            packed[(c, j)] = total
        return packed[(c, j)]

    copies = []
    for p in range(PARTS):
        for t in range(part // LANES):
            tile = p * (part // LANES) + t
            block, half = divmod(tile, WIDE // LANES)
            spans = [tile * TILE_SPANS + i for i in range(TILE_SPANS)]
            homes = [(s // span_cols, (s % span_cols) // SPANS_VREG) for s in spans]
            value = jnp.zeros((rows_dev, LANES), jnp.float32)
            for k in range(BLOCKS_KEPT):
                number = spread(rows[k], spans[0], at // SPAN_SIDE, spans[-1])
                got = None
                for s, home in zip(spans, homes):
                    if got is not None and home == homes[0]:
                        continue
                    base = s - home[0] * span_cols - home[1] * SPANS_VREG - (s - spans[0])
                    index = (base + at // SPAN_SIDE) * SLOT + k * BLOCK_SIDE + at % BLOCK_SIDE
                    new = take(vreg(*home), jnp.clip(index, 0, LANES - 1))
                    got = new if got is None else jnp.where(at >= (s - spans[0]) * SPAN_SIDE, new, got)
                hit = number % PER_SIDE == (at % SPAN_SIDE) // BLOCK_SIDE
                value = value + jnp.where(hit, got, 0.0)
            coeffs[block * rows_dev : (block + 1) * rows_dev, half * LANES : (half + 1) * LANES] = value
        tall = dot3(split(coeffs[p * stack : (p + 1) * stack, :]), wide)
        for i in range(part // WIDE):
            cut = (slice(None), slice(p * part + i * WIDE, p * part + (i + 1) * WIDE))
            result[cut] = decayed[cut] - tall[i * rows_dev : (i + 1) * rows_dev, :]
        cut = (slice(None), pl.ds(p * part, part))
        copies.append(pltpu.make_async_copy(result.at[cut], out.at[cut], sems.at[p]))
        copies[-1].start()
    for copy in copies:
        copy.wait()


def update_kernel(fsdp_count, every, sel_ref, wide_ref, square_ref, out, coeffs):
    replicas, span_rows = every.shape[:2]
    all_cols = sel_ref.shape[-1]
    span_cols = all_cols // fsdp_count
    rank = lax.axis_index("fsdp")
    replica = lax.axis_index("replica")
    wide = (wide_ref[0], wide_ref[1])
    square = (square_ref[0], square_ref[1])
    at = lane()
    first = rank * span_cols
    blocks = -(-span_cols * SPAN_SIDE // WIDE)
    tiles = -(-span_cols // TILE_SPANS)
    if tiles < blocks * (WIDE // LANES):
        coeffs[...] = jnp.zeros_like(coeffs)
    for r in range(span_rows):
        sums = [[None] * PER_SIDE for _ in range(tiles)]
        for q in range(replicas):
            rows = selection_rows(sel_ref[replica ^ q, r])
            for tile in range(tiles):
                span = tile * TILE_SPANS
                home = span // SPANS_VREG
                values = every[q, r, :, home * LANES : (home + 1) * LANES]
                offset = jnp.minimum(span + at // SPAN_SIDE, span_cols - 1)
                where = first + offset
                for k in range(BLOCKS_KEPT):
                    number = take(rows[k][0], where & (LANES - 1))
                    for v in range(1, len(rows[k])):
                        number = jnp.where(where >= v * LANES, take(rows[k][v], where & (LANES - 1)), number)
                    index = (span % SPANS_VREG + at // SPAN_SIDE) * SLOT + k * BLOCK_SIDE + at % BLOCK_SIDE
                    got = take(values, jnp.clip(index, 0, LANES - 1))
                    number = number - (at % SPAN_SIDE) // BLOCK_SIDE
                    for b in range(PER_SIDE):
                        hit = jnp.where(number == b * PER_SIDE, got, 0.0)
                        old = sums[tile][b]
                        sums[tile][b] = hit if old is None else old + hit
        for tile in range(tiles):
            block, half = divmod(tile, WIDE // LANES)
            for b in range(PER_SIDE):
                top = block * SPAN_SIDE + b * BLOCK_SIDE
                coeffs[top : top + BLOCK_SIDE, half * LANES : (half + 1) * LANES] = sums[tile][b]
        tall = dot3(split(coeffs[...]), wide)
        for i in range(blocks):
            piece = dot3(square, split(tall[i * SPAN_SIDE : (i + 1) * SPAN_SIDE, :]))
            stop = min(WIDE, span_cols * SPAN_SIDE - i * WIDE)
            out[r * SPAN_SIDE : (r + 1) * SPAN_SIDE, i * WIDE : i * WIDE + stop] = piece[:, :stop]


def swap(x, axis, bit):
    count = lax.axis_size(axis)
    return lax.ppermute(x, axis, [(i, i ^ bit) for i in range(count)])


def local(momentum, gradient, selection):
    fsdp_count = lax.axis_size("fsdp")
    replicas = lax.axis_size("replica")
    rank = lax.axis_index("fsdp")
    rows_dev, width = momentum.shape[1:]
    group = SPAN_SIDE // rows_dev
    span_rows = fsdp_count // group
    all_cols = width // SPAN_SIDE
    span_cols = all_cols // fsdp_count
    if rows_dev != BLOCK_SIDE or width % (PARTS * WIDE) or all_cols % fsdp_count:
        raise ValueError("unsupported sizes")
    packed = len(vregs_of(span_cols)) * LANES
    ahead_wide, back_wide, square, ahead, back = [jnp.asarray(t) for t in tables(rows_dev)]
    numbers = jnp.transpose(selection, (0, 1, 3, 2))
    vmem = pl.BlockSpec(memory_space=pltpu.VMEM)
    hbm = pl.BlockSpec(memory_space=pl.ANY)
    params = pltpu.CompilerParams(vmem_limit_bytes=16 * 1024 * 1024)
    tall = width // WIDE * rows_dev

    halves, decayed = pl.pallas_call(
        functools.partial(forward_kernel, fsdp_count),
        out_shape=[
            jax.ShapeDtypeStruct((2, fsdp_count // 2, BLOCK_SIDE, packed), jnp.float32),
            jax.ShapeDtypeStruct((rows_dev, width), jnp.float32),
        ],
        in_specs=[hbm, hbm, vmem, vmem, vmem],
        out_specs=[vmem, vmem],
        scratch_shapes=[
            pltpu.VMEM((rows_dev, width), jnp.float32),
            pltpu.VMEM((rows_dev, width), jnp.bfloat16),
            pltpu.VMEM((tall, WIDE), jnp.float32),
            pltpu.SemaphoreType.DMA((2, PARTS)),
        ],
        compiler_params=params,
        name="forward",
    )(momentum[0], gradient[0], numbers, ahead_wide, ahead)

    own = halves[0] + swap(halves[1], "fsdp", 1)
    for level in range(1, group.bit_length() - 1):
        own = own + swap(own, "fsdp", 1 << level)
    other = swap(own, "fsdp", 1)

    if span_rows == 1:
        mine = lax.dynamic_index_in_dim(own, rank // 2, 0, keepdims=True)
    else:
        spot = (jnp.arange(span_rows, dtype=jnp.int32) * group + rank % group) // 2
        mine = lax.all_to_all(
            own[spot], "fsdp", split_axis=0, concat_axis=0, tiled=True,
            axis_index_groups=[[g * group + m for g in range(span_rows)] for m in range(group)],
        )
    every = mine[None]
    for level in range(replicas.bit_length() - 1):
        every = jnp.concatenate([every, swap(every, "replica", 1 << level)], axis=0)

    residual = pl.pallas_call(
        functools.partial(residual_kernel, fsdp_count),
        out_shape=jax.ShapeDtypeStruct((rows_dev, width), jnp.float32),
        in_specs=[vmem] * 6,
        out_specs=hbm,
        scratch_shapes=[
            pltpu.VMEM((tall, WIDE), jnp.float32),
            pltpu.VMEM((rows_dev, width), jnp.float32),
            pltpu.SemaphoreType.DMA((PARTS,)),
        ],
        compiler_params=params,
        name="residual",
    )(decayed, own, other, numbers, back_wide, back)

    update = pl.pallas_call(
        functools.partial(update_kernel, fsdp_count),
        out_shape=jax.ShapeDtypeStruct((span_rows * SPAN_SIDE, span_cols * SPAN_SIDE), jnp.float32),
        in_specs=[vmem] * 4,
        out_specs=vmem,
        scratch_shapes=[pltpu.VMEM((-(-span_cols * SPAN_SIDE // WIDE) * SPAN_SIDE, WIDE), jnp.float32)],
        compiler_params=params,
        name="update",
    )(every, numbers, back_wide, square)
    return (residual[None], update)


def solution(mesh):
    specs = (P("replica", "fsdp", None), P("replica", "fsdp", None), P())
    return jax.shard_map(
        local,
        mesh=mesh,
        in_specs=specs,
        out_specs=(P("replica", "fsdp", None), P(None, "fsdp")),
        check_vma=False,
    )
```

```python
import functools
import types

import jax
import jax.numpy as jnp
import numpy as np
from jax import lax
from jax.experimental import pallas as pl
from jax.experimental.pallas import tpu as pltpu
from jax.sharding import PartitionSpec as P

SPAN_SIDE = 64
BLOCK_SIDE = 8
BLOCKS_KEPT = 2
PER_SIDE = SPAN_SIDE // BLOCK_SIDE
SLOT = BLOCKS_KEPT * BLOCK_SIDE
LANES = 128
WIDE = 256
SPANS_VREG = LANES // SLOT
TILE_SPANS = LANES // SPAN_SIDE
PARTS = 4

decay_rate = 0.9


def cosine_table():
    freq = np.arange(SPAN_SIDE, dtype=np.float64)[:, None]
    place = np.arange(SPAN_SIDE, dtype=np.float64)[None, :]
    scale = np.where(freq == 0, np.sqrt(1.0 / SPAN_SIDE), np.sqrt(2.0 / SPAN_SIDE))
    return scale * np.cos(np.pi * (2.0 * place + 1.0) * freq / (2.0 * SPAN_SIDE))


def np_split(x, terms):
    parts = []
    for _ in range(terms):
        parts.append(x.astype(np.float32).astype(jnp.bfloat16))
        x = x - parts[-1].astype(np.float64)
    return parts


def tables():
    cosine = cosine_table()
    blocks = np.kron(np.eye(WIDE // SPAN_SIDE), cosine)
    group = SPAN_SIDE // BLOCK_SIDE
    cut = cosine.reshape(SPAN_SIDE, group, BLOCK_SIDE).transpose(1, 0, 2)
    high, low = np_split(cut, 2)
    ahead = np.concatenate([high, low, high], axis=2)
    cut = cosine.reshape(PER_SIDE, BLOCK_SIDE, group, BLOCK_SIDE).transpose(2, 1, 3, 0)
    back = np.concatenate(np_split(cut.reshape(group, SPAN_SIDE, PER_SIDE), 3), axis=2)
    return (
        np.stack(np_split(blocks.T, 2)),
        np.stack(np_split(blocks, 2)),
        np.stack(np_split(cosine.T, 2)),
        ahead,
        back,
    )


def geometry(fsdp_count, rows_dev, width):
    g = types.SimpleNamespace(fsdp=fsdp_count, rows=rows_dev, width=width)
    g.group = SPAN_SIDE // rows_dev
    g.span_rows = fsdp_count // g.group
    g.cols = width // SPAN_SIDE
    g.span_cols = g.cols // fsdp_count
    g.bit = 0
    while (g.span_cols << g.bit) % TILE_SPANS:
        g.bit += 1
    g.seg = 1 << g.bit
    g.seg_spans = g.span_cols * g.seg
    g.seg_width = g.seg_spans * SPAN_SIDE
    g.segs = fsdp_count // 2 // g.seg
    g.half_spans = g.cols // 2
    g.half_tiles = g.half_spans // TILE_SPANS
    starts = [(((f >> (g.bit + 1)) << g.bit) | (f & (g.seg - 1))) * g.span_cols for f in range(fsdp_count)]
    g.window = max(-(-(s % SPANS_VREG + g.span_cols) // SPANS_VREG) for s in starts)
    g.vregs = max(-(-g.half_spans // SPANS_VREG), max(s // SPANS_VREG for s in starts) + g.window)
    g.tiles = -(-g.span_cols // TILE_SPANS)
    if rows_dev != BLOCK_SIDE or width % (PARTS * WIDE) or g.cols % fsdp_count or g.seg >= g.group:
        raise ValueError("unsupported sizes")
    return g


def span_of(g, half, spot):
    return ((spot // g.seg_spans) * 2 + half) * g.seg_spans + spot % g.seg_spans


def chunk_start(g, rank):
    place = (lax.shift_right_logical(rank, g.bit + 1) << g.bit) | (rank & (g.seg - 1))
    return place * g.span_cols


def split(x):
    high = x.astype(jnp.bfloat16)
    low = (x - high.astype(jnp.float32)).astype(jnp.bfloat16)
    return high, low


def dot(left, right):
    return jnp.dot(left, right, preferred_element_type=jnp.float32)


def dot3(left, right):
    return dot(left[0], right[0]) + (dot(left[1], right[0]) + dot(left[0], right[1]))


def take(x, index):
    return jnp.take_along_axis(x, index, axis=1, mode="promise_in_bounds")


def lane():
    return lax.broadcasted_iota(jnp.int32, (BLOCK_SIDE, LANES), 1)


def selection_rows(sel):
    count = sel.shape[1]
    full = -(-count // LANES) * LANES
    rows = []
    for k in range(BLOCKS_KEPT):
        row = sel[k : k + 1, :]
        if full != count:
            row = jnp.concatenate([row, jnp.zeros((1, full - count), jnp.int32)], axis=1)
        row = jnp.broadcast_to(row, (BLOCK_SIDE, full))
        rows.append([row[:, i : i + LANES] for i in range(0, full, LANES)])
    return rows


def packed_spans(g, half, v):
    spots = range(v * SPANS_VREG, min((v + 1) * SPANS_VREG, g.half_spans))
    spans = [span_of(g, half, s) for s in spots]
    if not spans:
        return [], None
    at = lane() // SLOT
    ids = spans[0] + at
    for n in range(1, len(spans)):
        jump = spans[n] - spans[n - 1] - 1
        if jump:
            ids = jnp.where(at >= n, ids + jump, ids)
    return spans, jnp.minimum(ids, max(spans)) if len(spans) < SPANS_VREG else ids


def forward_kernel(
    g, momentum, gradient, numbers, wide_hbm, table_hbm, out, decayed, marks,
    moment, grad, sel, wide_ref, table, coeffs, picked, sems,
):
    rank = lax.axis_index("fsdp")
    span_row, row_block = rank // g.group, rank % g.group
    part = g.width // PARTS
    small = [
        pltpu.make_async_copy(numbers.at[lax.axis_index("replica"), span_row], sel, sems.at[2, 0]),
        pltpu.make_async_copy(wide_hbm, wide_ref, sems.at[2, 1]),
        pltpu.make_async_copy(table_hbm.at[row_block], table, sems.at[2, 2]),
    ]
    for copy in small:
        copy.start()
    copies = []
    for p in range(PARTS):
        cut = (slice(None), pl.ds(p * part, part))
        for n, (src, dst) in enumerate(((momentum, moment), (gradient, grad))):
            copies.append(pltpu.make_async_copy(src.at[cut], dst.at[cut], sems.at[n, p]))
            copies[-1].start()
    at = lane()
    parity = lax.shift_right_logical(rank, g.bit) & 1
    small[0].wait()
    rows = selection_rows(sel[...])
    first_block = (at // BLOCK_SIDE) % BLOCKS_KEPT == 0
    todo = []
    for half in range(2):
        for v in range(g.vregs):
            spans, ids = packed_spans(g, half, v)
            if not spans:
                marks[half * g.vregs + v] = jnp.zeros(at.shape, jnp.int32)
                picked[:, (half * g.vregs + v) * LANES : (half * g.vregs + v + 1) * LANES] = jnp.zeros(
                    at.shape, jnp.float32
                )
                continue
            value = None
            for page in range(min(spans) // LANES, max(spans) // LANES + 1):
                local = ids & (LANES - 1)
                new = jnp.where(first_block, take(rows[0][page], local), take(rows[1][page], local))
                value = new if value is None else jnp.where(ids >= page * LANES, new, value)
            marks[half * g.vregs + v] = value
            todo.append((max(spans), half, v))
    todo.sort()
    small[1].wait()
    wide = (wide_ref[0], wide_ref[1])
    stack = part // WIDE * g.rows
    for p in range(PARTS):
        copies[2 * p].wait()
        copies[2 * p + 1].wait()
        cut = (slice(None), slice(p * part, (p + 1) * part))
        now = decay_rate * moment[cut] + grad[cut].astype(jnp.float32)
        decayed[cut] = now
        tall = jnp.concatenate([now[:, i : i + WIDE] for i in range(0, part, WIDE)], axis=0)
        coeffs[p * stack : (p + 1) * stack, :] = dot3(split(tall), wide)
        while todo and todo[0][0] < (p + 1) * part // SPAN_SIDE:
            _, half, v = todo.pop(0)
            spans, ids = packed_spans(g, half, v)
            index = (marks[half * g.vregs + v] % PER_SIDE) * BLOCK_SIDE + at % BLOCK_SIDE
            index = index + (ids % TILE_SPANS) * SPAN_SIDE
            value = None
            for tile in sorted({s // TILE_SPANS for s in spans}):
                block, side = divmod(tile, WIDE // LANES)
                new = coeffs[block * g.rows : (block + 1) * g.rows, side * LANES : (side + 1) * LANES]
                new = take(new, index)
                value = new if value is None else jnp.where(ids >= tile * TILE_SPANS, new, value)
            picked[:, (half * g.vregs + v) * LANES : (half * g.vregs + v + 1) * LANES] = value
    small[2].wait()
    kept = picked[...]
    high = kept.astype(jnp.bfloat16).astype(jnp.float32)
    three = jnp.concatenate([high, high, kept - high], axis=0).astype(jnp.bfloat16)
    tall = dot(table[...], three)
    for half in range(2):
        for v in range(g.vregs):
            n = half * g.vregs + v
            where = marks[n] // PER_SIDE
            value = tall[:BLOCK_SIDE, n * LANES : (n + 1) * LANES]
            for b in range(1, PER_SIDE):
                new = tall[b * BLOCK_SIDE : (b + 1) * BLOCK_SIDE, n * LANES : (n + 1) * LANES]
                value = jnp.where(where == b, new, value)
            out[half ^ parity, v] = value


def prepare_kernel(g, marks, table_ref, rows_out, masks):
    at = lane()
    up = lax.broadcasted_iota(jnp.int32, (BLOCK_SIDE, LANES), 0)
    table = table_ref[lax.axis_index("fsdp") % g.group]
    hot = jnp.concatenate(
        [jnp.where(marks[n] // PER_SIDE == up, 1.0, 0.0) for n in range(2 * g.vregs)], axis=1
    )
    hot = jnp.concatenate([hot, hot, hot], axis=0).astype(jnp.bfloat16)
    tall = dot(table, hot)
    for half in range(2):
        for v in range(g.vregs):
            n = half * g.vregs + v
            rows_out[half, v] = tall[:, n * LANES : (n + 1) * LANES]
    for spot in range(0, SPANS_VREG, TILE_SPANS):
        for k in range(BLOCKS_KEPT):
            index = (spot + at // SPAN_SIDE) * SLOT + k * BLOCK_SIDE + at % BLOCK_SIDE
            for half in range(2):
                for t in range(spot // TILE_SPANS, g.half_tiles, SPANS_VREG // TILE_SPANS):
                    number = take(marks[half * g.vregs + t * TILE_SPANS // SPANS_VREG], index)
                    hit = number % PER_SIDE == (at % SPAN_SIDE) // BLOCK_SIDE
                    masks[half, t, k] = jnp.where(hit, 1.0, 0.0)


def prepare_update_kernel(g, replicas, sel_ref, out):
    at = lane()
    rank = lax.axis_index("fsdp")
    replica = lax.axis_index("replica")
    first = rank * g.span_cols
    page, shift = first // LANES, first % LANES
    for r in range(g.span_rows):
        lined = []
        for q in range(replicas):
            for k, row in enumerate(selection_rows(sel_ref[replica ^ q, r])):
                low, high = row[0], row[-1]
                for n in range(1, len(row)):
                    low = jnp.where(page == n, row[n], low)
                    high = jnp.where(page == n - 1, row[n], high)
                turn = (LANES - shift) % LANES
                low, high = pltpu.roll(low, turn, 1), pltpu.roll(high, turn, 1)
                lined.append(jnp.where(at < LANES - shift, low, high))
        for t in range(g.tiles):
            index = jnp.minimum(t * TILE_SPANS + at // SPAN_SIDE, g.span_cols - 1)
            for n, row in enumerate(lined):
                out[r, n, t] = take(row, index) - (at % SPAN_SIDE) // BLOCK_SIDE


def half_residual(g, half, kept, rows_ref, masks, decayed, wide, coeffs, result):
    at = lane()
    inverse = []
    for v in range(-(-g.half_spans // SPANS_VREG)):
        total = None
        for i in range(BLOCK_SIDE):
            term = rows_ref[half, v, i * BLOCK_SIDE : (i + 1) * BLOCK_SIDE, :] * kept[v, i : i + 1, :]
            total = term if total is None else total + term
        inverse.append(total)
    for spot in range(0, SPANS_VREG, TILE_SPANS):
        tiles = range(spot // TILE_SPANS, g.half_tiles, SPANS_VREG // TILE_SPANS)
        values = {}
        for k in range(BLOCKS_KEPT):
            index = (spot + at // SPAN_SIDE) * SLOT + k * BLOCK_SIDE + at % BLOCK_SIDE
            for t in tiles:
                new = take(inverse[t * TILE_SPANS // SPANS_VREG], index) * masks[half, t, k]
                values[t] = new if k == 0 else values[t] + new
        for t in tiles:
            block, side = divmod(t, WIDE // LANES)
            coeffs[block * g.rows : (block + 1) * g.rows, side * LANES : (side + 1) * LANES] = values[t]
    tall = dot3(split(coeffs[...]), wide)
    seg_tiles = g.seg_width // LANES
    for t in range(g.half_tiles):
        block, side = divmod(t, WIDE // LANES)
        seg, inside = divmod(t, seg_tiles)
        column = (seg * 2 + half) * g.seg_width + inside * LANES
        was = decayed[:, pl.ds(pl.multiple_of(column, LANES), LANES)]
        piece = tall[block * g.rows : (block + 1) * g.rows, side * LANES : (side + 1) * LANES]
        result[:, t * LANES : (t + 1) * LANES] = was - piece


def half_copies(g, half, result, out, sems):
    copies = []
    for seg in range(g.segs):
        column = pl.multiple_of((seg * 2 + half) * g.seg_width, LANES)
        copies.append(
            pltpu.make_async_copy(
                result.at[:, pl.ds(seg * g.seg_width, g.seg_width)],
                out.at[:, pl.ds(column, g.seg_width)],
                sems.at[seg],
            )
        )
    return copies


def own_kernel(g, own, rows_ref, masks, decayed, wide_ref, out, coeffs, result, sems):
    half = lax.shift_right_logical(lax.axis_index("fsdp"), g.bit) & 1
    half_residual(g, half, own, rows_ref, masks, decayed, (wide_ref[0], wide_ref[1]), coeffs, result)
    copies = half_copies(g, half, result, out, sems)
    for copy in copies:
        copy.start()
    for copy in copies:
        copy.wait()


def finish_kernel(
    g, replicas, started, other, rows_ref, masks, decayed, wide_ref, every, numbers, square_ref,
    residual, update, coeffs, result, sums_ref, update_ref, sems, update_sems,
):
    del started
    rank = lax.axis_index("fsdp")
    half = (lax.shift_right_logical(rank, g.bit) & 1) ^ 1
    wide = (wide_ref[0], wide_ref[1])
    half_residual(g, half, other, rows_ref, masks, decayed, wide, coeffs, result)
    copies = half_copies(g, half, result, residual, sems)
    for copy in copies:
        copy.start()

    at = lane()
    square = (square_ref[0], square_ref[1])
    start = chunk_start(g, rank)
    shift = (start % SPANS_VREG) * SLOT
    turn = (LANES - shift) % LANES
    blocks = -(-g.tiles // (WIDE // LANES))
    for r in range(g.span_rows):
        lined = []
        for q in range(replicas):
            turned = [pltpu.roll(every[q, r, v], turn, 1) for v in range(g.window)]
            turned.append(turned[-1])
            lined.append([jnp.where(at < LANES - shift, turned[v], turned[v + 1]) for v in range(g.window)])
        for t in range(blocks * (WIDE // LANES)):
            sums = [None] * PER_SIDE
            if t < g.tiles:
                spot = t * TILE_SPANS % SPANS_VREG
                for k in range(BLOCKS_KEPT):
                    index = (spot + at // SPAN_SIDE) * SLOT + k * BLOCK_SIDE + at % BLOCK_SIDE
                    for q in range(replicas):
                        got = take(lined[q][t * TILE_SPANS // SPANS_VREG], index)
                        number = numbers[r, q * BLOCKS_KEPT + k, t]
                        for b in range(PER_SIDE):
                            new = jnp.where(number == b * PER_SIDE, got, 0.0)
                            sums[b] = new if sums[b] is None else sums[b] + new
            block, side = divmod(t, WIDE // LANES)
            for b in range(PER_SIDE):
                top = block * SPAN_SIDE + b * BLOCK_SIDE
                value = jnp.zeros(at.shape, jnp.float32) if sums[b] is None else sums[b]
                sums_ref[top : top + BLOCK_SIDE, side * LANES : (side + 1) * LANES] = value
        tall = dot3(split(sums_ref[...]), wide)
        for i in range(blocks):
            piece = dot3(square, split(tall[i * SPAN_SIDE : (i + 1) * SPAN_SIDE, :]))
            stop = min(WIDE, g.span_cols * SPAN_SIDE - i * WIDE)
            update_ref[r * SPAN_SIDE : (r + 1) * SPAN_SIDE, i * WIDE : i * WIDE + stop] = piece[:, :stop]
        cut = pl.ds(r * SPAN_SIDE, SPAN_SIDE)
        copies.append(pltpu.make_async_copy(update_ref.at[cut], update.at[cut], update_sems.at[r]))
        copies[-1].start()
    for copy in copies:
        copy.wait()


def swap(x, axis, bit):
    count = lax.axis_size(axis)
    return lax.ppermute(x, axis, [(i, i ^ bit) for i in range(count)])


def call(kernel, name, out_shape, in_specs, out_specs, scratch=(), flops=0, **options):
    return pl.pallas_call(
        kernel,
        out_shape=out_shape,
        in_specs=in_specs,
        out_specs=out_specs,
        scratch_shapes=list(scratch),
        compiler_params=pltpu.CompilerParams(vmem_limit_bytes=12 * 1024 * 1024),
        cost_estimate=pl.CostEstimate(flops=flops, bytes_accessed=1 << 20, transcendentals=0),
        name=name,
        **options,
    )


def local(momentum, gradient, selection):
    replicas = lax.axis_size("replica")
    rank = lax.axis_index("fsdp")
    g = geometry(lax.axis_size("fsdp"), *momentum.shape[1:])
    ahead_wide, back_wide, square, ahead, back = [jnp.asarray(t) for t in tables()]
    numbers = jnp.transpose(selection, (0, 1, 3, 2))
    vmem = pl.BlockSpec(memory_space=pltpu.VMEM)
    hbm = pl.BlockSpec(memory_space=pltpu.HBM)
    f32 = functools.partial(jax.ShapeDtypeStruct, dtype=jnp.float32)
    i32 = functools.partial(jax.ShapeDtypeStruct, dtype=jnp.int32)
    tall = g.width // WIDE * g.rows
    half_tall = -(-g.half_tiles // (WIDE // LANES)) * g.rows
    dma = pltpu.SemaphoreType.DMA
    tile = (BLOCK_SIDE, LANES)

    halves, decayed, marks = call(
        functools.partial(forward_kernel, g),
        "forward",
        [f32((2, g.vregs) + tile), f32((g.rows, g.width)), i32((2 * g.vregs,) + tile)],
        [hbm] * 5,
        [vmem] * 3,
        [
            pltpu.VMEM((g.rows, g.width), jnp.float32),
            pltpu.VMEM((g.rows, g.width), jnp.bfloat16),
            pltpu.VMEM((BLOCKS_KEPT, g.cols), jnp.int32),
            pltpu.VMEM(ahead_wide.shape, jnp.bfloat16),
            pltpu.VMEM(ahead.shape[1:], jnp.bfloat16),
            pltpu.VMEM((tall, WIDE), jnp.float32),
            pltpu.VMEM((BLOCK_SIDE, 2 * g.vregs * LANES), jnp.float32),
            dma((3, PARTS)),
        ],
        flops=10**9,
    )(*[pltpu.with_memory_space_constraint(x, pltpu.HBM) for x in (momentum[0], gradient[0], numbers, ahead_wide, ahead)])

    rows, masks = call(
        functools.partial(prepare_kernel, g),
        "prepare",
        [f32((2, g.vregs, SPAN_SIDE, LANES)), f32((2, g.half_tiles, BLOCKS_KEPT) + tile)],
        [vmem] * 2,
        [vmem] * 2,
        flops=10**9,
    )(marks, back)
    places = call(
        functools.partial(prepare_update_kernel, g, replicas),
        "prepare_update",
        i32((g.span_rows, replicas * BLOCKS_KEPT, g.tiles) + tile),
        [vmem],
        vmem,
        flops=10**9,
    )(numbers)

    own = halves[0] + swap(halves[1], "fsdp", g.seg)
    own, rows, masks = lax.optimization_barrier((own, rows, masks))
    for level in range(g.group.bit_length() - 1):
        if level != g.bit:
            own = own + swap(own, "fsdp", 1 << level)
            own, places = lax.optimization_barrier((own, places))
    other = swap(own, "fsdp", g.seg)

    if g.span_rows == 1:
        mine = lax.dynamic_slice_in_dim(own, chunk_start(g, rank) // SPANS_VREG, g.window, 0)[None]
    else:
        ranks = [rank % g.group + s * g.group for s in range(g.span_rows)]
        pieces = [lax.dynamic_slice_in_dim(own, chunk_start(g, f) // SPANS_VREG, g.window, 0) for f in ranks]
        mine = lax.all_to_all(
            jnp.stack(pieces), "fsdp", split_axis=0, concat_axis=0, tiled=True,
            axis_index_groups=[[s * g.group + m for s in range(g.span_rows)] for m in range(g.group)],
        )
    every = mine[None]
    for level in range(replicas.bit_length() - 1):
        every = jnp.concatenate([every, swap(every, "replica", 1 << level)], axis=0)

    half_scratch = [
        pltpu.VMEM((half_tall, WIDE), jnp.float32),
        pltpu.VMEM((g.rows, g.half_tiles * LANES), jnp.float32),
    ]
    started = call(
        functools.partial(own_kernel, g),
        "own",
        f32((g.rows, g.width)),
        [vmem] * 5,
        hbm,
        half_scratch + [dma((g.segs,))],
        flops=10**9,
    )(own, rows, masks, decayed, back_wide)

    high, wide = g.span_rows * SPAN_SIDE, g.span_cols * SPAN_SIDE
    residual, update = call(
        functools.partial(finish_kernel, g, replicas),
        "finish",
        [f32((g.rows, g.width)), f32((high, wide))],
        [hbm] + [vmem] * 8,
        [hbm] * 2,
        half_scratch
        + [
            pltpu.VMEM((-(-wide // WIDE) * SPAN_SIDE, WIDE), jnp.float32),
            pltpu.VMEM((high, wide), jnp.float32),
            dma((g.segs,)),
            dma((g.span_rows,)),
        ],
        flops=10**9,
        input_output_aliases={0: 0},
    )(started, other, rows, masks, decayed, back_wide, every, places, square)
    return (residual[None], update)


def solution(mesh):
    specs = (P("replica", "fsdp", None), P("replica", "fsdp", None), P())
    return jax.shard_map(
        local,
        mesh=mesh,
        in_specs=specs,
        out_specs=(P("replica", "fsdp", None), P(None, "fsdp")),
        check_vma=False,
    )
```

```python
import functools
import types

import jax
import jax.numpy as jnp
import numpy as np
from jax import lax
from jax.experimental import pallas as pl
from jax.experimental.pallas import tpu as pltpu
from jax.sharding import PartitionSpec as P


SPAN_SIDE = 64
BLOCK_SIDE = 8
BLOCKS_KEPT = 2
PER_SIDE = SPAN_SIDE // BLOCK_SIDE
SLOT = BLOCKS_KEPT * BLOCK_SIDE
LANES = 128
WIDE = 256
SPANS_VREG = LANES // SLOT
TILE_SPANS = LANES // SPAN_SIDE
PARTS = 4

decay_rate = 0.9


def cosine_table():
    freq = np.arange(SPAN_SIDE, dtype=np.float64)[:, None]
    place = np.arange(SPAN_SIDE, dtype=np.float64)[None, :]
    scale = np.where(freq == 0, np.sqrt(1.0 / SPAN_SIDE), np.sqrt(2.0 / SPAN_SIDE))
    return scale * np.cos(np.pi * (2.0 * place + 1.0) * freq / (2.0 * SPAN_SIDE))


def np_split(x, terms):
    parts = []
    for _ in range(terms):
        parts.append(x.astype(np.float32).astype(jnp.bfloat16))
        x = x - parts[-1].astype(np.float64)
    return parts


def tables():
    cosine = cosine_table()
    blocks = np.kron(np.eye(WIDE // SPAN_SIDE), cosine)
    group = SPAN_SIDE // BLOCK_SIDE
    cut = cosine.reshape(SPAN_SIDE, group, BLOCK_SIDE).transpose(1, 0, 2)
    high, low = np_split(cut, 2)
    ahead = np.concatenate([high, low, high], axis=2)
    cut = cosine.reshape(PER_SIDE, BLOCK_SIDE, group, BLOCK_SIDE).transpose(2, 1, 3, 0)
    back = np.concatenate(np_split(cut.reshape(group, SPAN_SIDE, PER_SIDE), 3), axis=2)
    return (
        np.stack(np_split(blocks.T, 2)),
        np.stack(np_split(blocks, 2)),
        np.concatenate([*np_split(cosine.T, 2), np_split(cosine.T, 1)[0]], axis=1),
        ahead,
        back,
    )


def geometry(fsdp_count, rows_dev, width):
    g = types.SimpleNamespace(fsdp=fsdp_count, rows=rows_dev, width=width)
    g.group = SPAN_SIDE // rows_dev
    g.span_rows = fsdp_count // g.group
    g.cols = width // SPAN_SIDE
    g.span_cols = g.cols // fsdp_count
    g.bit = 0
    while (g.span_cols << g.bit) % TILE_SPANS:
        g.bit += 1
    g.seg = 1 << g.bit
    g.seg_spans = g.span_cols * g.seg
    g.seg_width = g.seg_spans * SPAN_SIDE
    g.segs = fsdp_count // 2 // g.seg
    g.half_spans = g.cols // 2
    g.half_tiles = g.half_spans // TILE_SPANS
    starts = [(((f >> (g.bit + 1)) << g.bit) | (f & (g.seg - 1))) * g.span_cols for f in range(fsdp_count)]
    g.window = max(-(-(s % SPANS_VREG + g.span_cols) // SPANS_VREG) for s in starts)
    g.vregs = max(-(-g.half_spans // SPANS_VREG), max(s // SPANS_VREG for s in starts) + g.window)
    g.tiles = -(-g.span_cols // TILE_SPANS)
    if rows_dev != BLOCK_SIDE or width % (PARTS * WIDE) or g.cols % fsdp_count or g.seg >= g.group:
        raise ValueError("unsupported sizes")
    return g


def span_of(g, half, spot):
    return ((spot // g.seg_spans) * 2 + half) * g.seg_spans + spot % g.seg_spans


def chunk_start(g, rank):
    place = (lax.shift_right_logical(rank, g.bit + 1) << g.bit) | (rank & (g.seg - 1))
    return place * g.span_cols


def split(x):
    high = x.astype(jnp.bfloat16)
    low = (x - high.astype(jnp.float32)).astype(jnp.bfloat16)
    return high, low


def dot(left, right):
    return jnp.dot(left, right, preferred_element_type=jnp.float32)


def dot3(left, right):
    return dot(left[0], right[0]) + (dot(left[1], right[0]) + dot(left[0], right[1]))


def take(x, index):
    return jnp.take_along_axis(x, index, axis=1, mode="promise_in_bounds")


def lane():
    return lax.broadcasted_iota(jnp.int32, (BLOCK_SIDE, LANES), 1)


def selection_rows(sel):
    count = sel.shape[1]
    full = -(-count // LANES) * LANES
    rows = []
    for k in range(BLOCKS_KEPT):
        row = sel[k : k + 1, :]
        if full != count:
            row = jnp.concatenate([row, jnp.zeros((1, full - count), jnp.int32)], axis=1)
        row = jnp.broadcast_to(row, (BLOCK_SIDE, full))
        rows.append([row[:, i : i + LANES] for i in range(0, full, LANES)])
    return rows


def packed_spans(g, half, v):
    spots = range(v * SPANS_VREG, min((v + 1) * SPANS_VREG, g.half_spans))
    spans = [span_of(g, half, s) for s in spots]
    if not spans:
        return [], None
    at = lane() // SLOT
    ids = spans[0] + at
    for n in range(1, len(spans)):
        jump = spans[n] - spans[n - 1] - 1
        if jump:
            ids = jnp.where(at >= n, ids + jump, ids)
    return spans, jnp.minimum(ids, max(spans)) if len(spans) < SPANS_VREG else ids


def forward_kernel(
    g, momentum, gradient, numbers, wide_hbm, table_hbm, out, decayed, marks,
    moment, grad, sel, wide_ref, table, coeffs, picked, sems,
):
    rank = lax.axis_index("fsdp")
    span_row, row_block = rank // g.group, rank % g.group
    part = g.width // PARTS
    small = [
        pltpu.make_async_copy(numbers.at[lax.axis_index("replica"), span_row], sel, sems.at[2, 0]),
        pltpu.make_async_copy(wide_hbm, wide_ref, sems.at[2, 1]),
        pltpu.make_async_copy(table_hbm.at[row_block], table, sems.at[2, 2]),
    ]
    for copy in small:
        copy.start()
    copies = []
    for p in range(PARTS):
        cut = (slice(None), pl.ds(p * part, part))
        for n, (src, dst) in enumerate(((momentum, moment), (gradient, grad))):
            copies.append(pltpu.make_async_copy(src.at[cut], dst.at[cut], sems.at[n, p]))
            copies[-1].start()
    at = lane()
    parity = lax.shift_right_logical(rank, g.bit) & 1
    small[0].wait()
    rows = selection_rows(sel[...])
    first_block = (at // BLOCK_SIDE) % BLOCKS_KEPT == 0
    todo = []
    for half in range(2):
        for v in range(g.vregs):
            spans, ids = packed_spans(g, half, v)
            if not spans:
                marks[half * g.vregs + v] = jnp.zeros(at.shape, jnp.int32)
                picked[:, (half * g.vregs + v) * LANES : (half * g.vregs + v + 1) * LANES] = jnp.zeros(
                    at.shape, jnp.float32
                )
                continue
            value = None
            for page in range(min(spans) // LANES, max(spans) // LANES + 1):
                local = ids & (LANES - 1)
                new = jnp.where(first_block, take(rows[0][page], local), take(rows[1][page], local))
                value = new if value is None else jnp.where(ids >= page * LANES, new, value)
            marks[half * g.vregs + v] = value
            todo.append((max(spans), half, v))
    todo.sort()
    small[1].wait()
    wide = (wide_ref[0], wide_ref[1])
    stack = part // WIDE * g.rows
    for p in range(PARTS + 1):
        if p < PARTS:
            copies[2 * p].wait()
            copies[2 * p + 1].wait()
            cut = (slice(None), slice(p * part, (p + 1) * part))
            now = decay_rate * moment[cut] + grad[cut].astype(jnp.float32)
            decayed[cut] = now
            tall = jnp.concatenate([now[:, i : i + WIDE] for i in range(0, part, WIDE)], axis=0)
            tall = dot3(split(tall), wide)
        while todo and todo[0][0] < p * part // SPAN_SIDE:
            _, half, v = todo.pop(0)
            spans, ids = packed_spans(g, half, v)
            index = (marks[half * g.vregs + v] % PER_SIDE) * BLOCK_SIDE + at % BLOCK_SIDE
            index = index + (ids % TILE_SPANS) * SPAN_SIDE
            value = None
            for tile in sorted({s // TILE_SPANS for s in spans}):
                block, side = divmod(tile, WIDE // LANES)
                new = coeffs[block * g.rows : (block + 1) * g.rows, side * LANES : (side + 1) * LANES]
                new = take(new, index)
                value = new if value is None else jnp.where(ids >= tile * TILE_SPANS, new, value)
            picked[:, (half * g.vregs + v) * LANES : (half * g.vregs + v + 1) * LANES] = value
        if p < PARTS:
            coeffs[p * stack : (p + 1) * stack, :] = tall
    small[2].wait()
    kept = picked[...]
    high = kept.astype(jnp.bfloat16).astype(jnp.float32)
    three = jnp.concatenate([high, high, kept - high], axis=0).astype(jnp.bfloat16)
    tall = dot(table[...], three)
    for half in range(2):
        for v in range(g.vregs):
            n = half * g.vregs + v
            where = marks[n] // PER_SIDE
            value = tall[:BLOCK_SIDE, n * LANES : (n + 1) * LANES]
            for b in range(1, PER_SIDE):
                new = tall[b * BLOCK_SIDE : (b + 1) * BLOCK_SIDE, n * LANES : (n + 1) * LANES]
                value = jnp.where(where == b, new, value)
            out[half ^ parity, v] = value


def prepare_kernel(g, marks, table_ref, rows_out, masks):
    at = lane()
    up = lax.broadcasted_iota(jnp.int32, (BLOCK_SIDE, LANES), 0)
    table = table_ref[lax.axis_index("fsdp") % g.group]
    hot = jnp.concatenate(
        [jnp.where(marks[n] // PER_SIDE == up, 1.0, 0.0) for n in range(2 * g.vregs)], axis=1
    )
    hot = jnp.concatenate([hot, hot, hot], axis=0).astype(jnp.bfloat16)
    tall = dot(table, hot)
    for half in range(2):
        for v in range(g.vregs):
            n = half * g.vregs + v
            rows_out[half, v] = tall[:, n * LANES : (n + 1) * LANES]
    for spot in range(0, SPANS_VREG, TILE_SPANS):
        for k in range(BLOCKS_KEPT):
            index = (spot + at // SPAN_SIDE) * SLOT + k * BLOCK_SIDE + at % BLOCK_SIDE
            for half in range(2):
                for t in range(spot // TILE_SPANS, g.half_tiles, SPANS_VREG // TILE_SPANS):
                    number = take(marks[half * g.vregs + t * TILE_SPANS // SPANS_VREG], index)
                    hit = number % PER_SIDE == (at % SPAN_SIDE) // BLOCK_SIDE
                    masks[half, t, k] = jnp.where(hit, 1.0, 0.0)


def prepare_update_kernel(g, replicas, sel_ref, out):
    at = lane()
    rank = lax.axis_index("fsdp")
    replica = lax.axis_index("replica")
    first = rank * g.span_cols
    page, shift = first // LANES, first % LANES
    for r in range(g.span_rows):
        lined = []
        for q in range(replicas):
            for row in selection_rows(sel_ref[replica ^ q, r]):
                low, high = row[0], row[-1]
                for n in range(1, len(row)):
                    low = jnp.where(page == n, row[n], low)
                    high = jnp.where(page == n - 1, row[n], high)
                turn = (LANES - shift) % LANES
                low, high = pltpu.roll(low, turn, 1), pltpu.roll(high, turn, 1)
                lined.append(jnp.where(at < LANES - shift, low, high))
        for t in range(g.tiles):
            index = jnp.minimum(t * TILE_SPANS + at // SPAN_SIDE, g.span_cols - 1)
            for n, row in enumerate(lined):
                out[r, n, t] = take(row, index) - (at % SPAN_SIDE) // BLOCK_SIDE


def half_residual(g, half, kept, rows_ref, masks, decayed, wide, coeffs, result):
    at = lane()
    inverse = []
    for v in range(-(-g.half_spans // SPANS_VREG)):
        total = None
        for i in range(BLOCK_SIDE):
            term = rows_ref[half, v, i * BLOCK_SIDE : (i + 1) * BLOCK_SIDE, :] * kept[v, i : i + 1, :]
            total = term if total is None else total + term
        inverse.append(total)
    for spot in range(0, SPANS_VREG, TILE_SPANS):
        tiles = range(spot // TILE_SPANS, g.half_tiles, SPANS_VREG // TILE_SPANS)
        values = {}
        for k in range(BLOCKS_KEPT):
            index = (spot + at // SPAN_SIDE) * SLOT + k * BLOCK_SIDE + at % BLOCK_SIDE
            for t in tiles:
                new = take(inverse[t * TILE_SPANS // SPANS_VREG], index) * masks[half, t, k]
                values[t] = new if k == 0 else values[t] + new
        for t in tiles:
            block, side = divmod(t, WIDE // LANES)
            coeffs[block * g.rows : (block + 1) * g.rows, side * LANES : (side + 1) * LANES] = values[t]
    tall = dot3(split(coeffs[...]), wide)
    seg_tiles = g.seg_width // LANES
    for t in range(g.half_tiles):
        block, side = divmod(t, WIDE // LANES)
        seg, inside = divmod(t, seg_tiles)
        column = (seg * 2 + half) * g.seg_width + inside * LANES
        was = decayed[:, pl.ds(pl.multiple_of(column, LANES), LANES)]
        piece = tall[block * g.rows : (block + 1) * g.rows, side * LANES : (side + 1) * LANES]
        result[:, t * LANES : (t + 1) * LANES] = was - piece


def half_kernel(g, flip, kept, rows_ref, masks, decayed, wide_ref, result, coeffs):
    half = (lax.shift_right_logical(lax.axis_index("fsdp"), g.bit) & 1) ^ flip
    half_residual(g, half, kept, rows_ref, masks, decayed, (wide_ref[0], wide_ref[1]), coeffs, result)


def half_copies(g, half, result, out, sems):
    copies = []
    for seg in range(g.segs):
        column = pl.multiple_of((seg * 2 + half) * g.seg_width, LANES)
        copies.append(
            pltpu.make_async_copy(
                result.at[:, pl.ds(seg * g.seg_width, g.seg_width)],
                out.at[:, pl.ds(column, g.seg_width)],
                sems.at[seg],
            )
        )
    return copies


def lined_up(g, every, r):
    at = lane()
    shift = (chunk_start(g, lax.axis_index("fsdp")) % SPANS_VREG) * SLOT
    turn = (LANES - shift) % LANES
    lined = []
    for q in range(every.shape[0]):
        turned = [pltpu.roll(every[q, r, v], turn, 1) for v in range(g.window)]
        turned.append(turned[-1])
        lined.append([jnp.where(at < LANES - shift, turned[v], turned[v + 1]) for v in range(g.window)])
    return lined


def tile_sums(lined, numbers, r, base, t):
    at = lane()
    sums = [None] * PER_SIDE
    for k in range(BLOCKS_KEPT):
        index = (t * TILE_SPANS % SPANS_VREG + at // SPAN_SIDE) * SLOT + k * BLOCK_SIDE + at % BLOCK_SIDE
        for q, row in enumerate(lined):
            got = take(row[t * TILE_SPANS // SPANS_VREG], index)
            number = numbers[r, (base + q) * BLOCKS_KEPT + k, t]
            for b in range(PER_SIDE):
                new = jnp.where(number == b * PER_SIDE, got, 0.0)
                sums[b] = new if sums[b] is None else sums[b] + new
    return sums


def sum_kernel(g, every, numbers, out):
    for r in range(g.span_rows):
        lined = lined_up(g, every, r)
        for t in range(g.tiles):
            for b, value in enumerate(tile_sums(lined, numbers, r, 0, t)):
                out[r, t, b] = value


def update_kernel(
    g, own, other, sums, every, numbers, wide_ref, square_ref,
    residual, update, sums_ref, update_ref, sems, update_sems,
):
    half = lax.shift_right_logical(lax.axis_index("fsdp"), g.bit) & 1
    copies = half_copies(g, half, own, residual, sems.at[0]) + half_copies(g, half ^ 1, other, residual, sems.at[1])
    for copy in copies:
        copy.start()
    wide = (wide_ref[0], wide_ref[1])
    square = square_ref[...]
    base = every.shape[0]
    pair = WIDE // LANES
    for r in range(g.span_rows):
        lined = lined_up(g, every, r)
        for i in range(-(-g.tiles // pair)):
            for t in range(i * pair, (i + 1) * pair):
                values = tile_sums(lined, numbers, r, base, t) if t < g.tiles else None
                for b in range(PER_SIDE):
                    value = jnp.zeros((BLOCK_SIDE, LANES), jnp.float32) if values is None else values[b] + sums[r, t, b]
                    side = t % pair
                    sums_ref[i, b * BLOCK_SIDE : (b + 1) * BLOCK_SIDE, side * LANES : (side + 1) * LANES] = value
        stack = jnp.concatenate([sums_ref[i] for i in range(-(-g.tiles // pair))], axis=0)
        tall = dot3(split(stack), wide)
        for i in range(-(-g.tiles // pair)):
            high, low = split(tall[i * SPAN_SIDE : (i + 1) * SPAN_SIDE, :])
            piece = dot(square, jnp.concatenate([high, high, low], axis=0))
            stop = min(WIDE, g.span_cols * SPAN_SIDE - i * WIDE)
            rows = slice(r * SPAN_SIDE, (r + 1) * SPAN_SIDE)
            update_ref[rows, i * WIDE : i * WIDE + stop] = piece[:, :stop]
        cut = pl.ds(r * SPAN_SIDE, SPAN_SIDE)
        copies.append(pltpu.make_async_copy(update_ref.at[cut], update.at[cut], update_sems.at[r]))
        copies[-1].start()
    for copy in copies:
        copy.wait()


def swap(x, axis, bit):
    count = lax.axis_size(axis)
    return lax.ppermute(x, axis, [(i, i ^ bit) for i in range(count)])


def call(kernel, out_shape, in_specs, out_specs, scratch=(), flops=0, **options):
    return pl.pallas_call(
        kernel,
        out_shape=out_shape,
        in_specs=in_specs,
        out_specs=out_specs,
        scratch_shapes=list(scratch),
        compiler_params=pltpu.CompilerParams(vmem_limit_bytes=12 * 1024 * 1024),
        cost_estimate=pl.CostEstimate(flops=flops, bytes_accessed=1 << 20, transcendentals=0),
        **options,
    )


def step(momentum, gradient, selection):
    replicas = lax.axis_size("replica")
    rank = lax.axis_index("fsdp")
    g = geometry(lax.axis_size("fsdp"), *momentum.shape[1:])
    ahead_wide, back_wide, square, ahead, back = [jnp.asarray(t) for t in tables()]
    numbers = jnp.transpose(selection, (0, 1, 3, 2))
    vmem = pl.BlockSpec(memory_space=pltpu.VMEM)
    hbm = pl.BlockSpec(memory_space=pltpu.HBM)
    f32 = functools.partial(jax.ShapeDtypeStruct, dtype=jnp.float32)
    i32 = functools.partial(jax.ShapeDtypeStruct, dtype=jnp.int32)
    tall = g.width // WIDE * g.rows
    half_tall = -(-g.half_tiles // (WIDE // LANES)) * g.rows
    dma = pltpu.SemaphoreType.DMA
    tile = (BLOCK_SIDE, LANES)

    halves, decayed, marks = call(
        functools.partial(forward_kernel, g),
        [f32((2, g.vregs) + tile), f32((g.rows, g.width)), i32((2 * g.vregs,) + tile)],
        [hbm] * 5,
        [vmem] * 3,
        [
            pltpu.VMEM((g.rows, g.width), jnp.float32),
            pltpu.VMEM((g.rows, g.width), jnp.bfloat16),
            pltpu.VMEM((BLOCKS_KEPT, g.cols), jnp.int32),
            pltpu.VMEM(ahead_wide.shape, jnp.bfloat16),
            pltpu.VMEM(ahead.shape[1:], jnp.bfloat16),
            pltpu.VMEM((tall, WIDE), jnp.float32),
            pltpu.VMEM((BLOCK_SIDE, 2 * g.vregs * LANES), jnp.float32),
            dma((3, PARTS)),
        ],
        flops=10**9,
    )(*[pltpu.with_memory_space_constraint(x, pltpu.HBM) for x in (momentum[0], gradient[0], numbers, ahead_wide, ahead)])

    rows, masks = call(
        functools.partial(prepare_kernel, g),
        [f32((2, g.vregs, SPAN_SIDE, LANES)), f32((2, g.half_tiles, BLOCKS_KEPT) + tile)],
        [vmem] * 2,
        [vmem] * 2,
        flops=10**9,
    )(marks, back)
    places = call(
        functools.partial(prepare_update_kernel, g, replicas),
        i32((g.span_rows, replicas * BLOCKS_KEPT, g.tiles) + tile),
        [vmem],
        vmem,
        flops=10**9,
    )(numbers)

    levels = [1 << n for n in range(g.group.bit_length() - 1) if n != g.bit]
    keep, send = halves[0], halves[1]
    own = keep + swap(send, "fsdp", g.seg)
    if levels:
        own = own + swap(keep, "fsdp", levels[0]) + swap(send, "fsdp", levels[0] | g.seg)
    own, rows, masks, places = lax.optimization_barrier((own, rows, masks, places))
    for level in levels[1:]:
        own = own + swap(own, "fsdp", level)
    other = swap(own, "fsdp", g.seg)

    if g.span_rows == 1:
        mine = lax.dynamic_slice_in_dim(own, chunk_start(g, rank) // SPANS_VREG, g.window, 0)[None]
    else:
        ranks = [rank % g.group + s * g.group for s in range(g.span_rows)]
        pieces = [lax.dynamic_slice_in_dim(own, chunk_start(g, f) // SPANS_VREG, g.window, 0) for f in ranks]
        mine = lax.all_to_all(
            jnp.stack(pieces), "fsdp", split_axis=0, concat_axis=0, tiled=True,
            axis_index_groups=[[s * g.group + m for s in range(g.span_rows)] for m in range(g.group)],
        )
    first = mine[None]
    levels = [1 << n for n in range(replicas.bit_length() - 1)]
    for level in levels[:-1]:
        first = jnp.concatenate([first, swap(first, "replica", level)], axis=0)
    last = swap(first, "replica", levels[-1])

    def residual_half(flip, kept):
        return call(
            functools.partial(half_kernel, g, flip),
            f32((g.rows, g.half_tiles * LANES)),
            [vmem] * 5,
            vmem,
            [pltpu.VMEM((half_tall, WIDE), jnp.float32)],
            flops=10**9,
        )(kept, rows, masks, decayed, back_wide)

    own_half = residual_half(0, own)
    other_half = residual_half(1, other)
    sums = call(
        functools.partial(sum_kernel, g), f32((g.span_rows, g.tiles, PER_SIDE) + tile), [vmem] * 2, vmem, flops=10**9
    )(first, places)
    high, wide = g.span_rows * SPAN_SIDE, g.span_cols * SPAN_SIDE
    residual, update = call(
        functools.partial(update_kernel, g),
        [f32((g.rows, g.width)), f32((high, wide))],
        [vmem] * 7,
        [hbm] * 2,
        [
            pltpu.VMEM((-(-wide // WIDE), SPAN_SIDE, WIDE), jnp.float32),
            pltpu.VMEM((high, wide), jnp.float32),
            dma((2, g.segs)),
            dma((g.span_rows,)),
        ],
        flops=10**9,
    )(own_half, other_half, sums, last, places, back_wide, square)
    return (residual[None], update)


def solution(mesh):
    specs = (P("replica", "fsdp", None), P("replica", "fsdp", None), P())
    return jax.shard_map(
        step,
        mesh=mesh,
        in_specs=specs,
        out_specs=(P("replica", "fsdp", None), P(None, "fsdp")),
        check_vma=False,
    )
```
